128 devices in a mesh: wide: 64 (over y, z, x), narrow: 2 (over core).
Axes of the slice: x: 4, y: 4, z: 4, core: 2. Of those that a mesh axis runs over, the one named last changes fastest.
Arguments:
- tokens: bfloat16 [16384, 4096], P(('wide', 'narrow')), may hold values from -6 to 6
- expert_ids: int32 [16384, 2], P(('wide', 'narrow')), may hold values from 0 to 127, all different within a row; in each aligned block of 128 rows (0 to 127, 128 to 255, ...) at most 3 rows name the same one
- gate_values: bfloat16 [16384, 2], P(('wide', 'narrow')), may hold values from 0.099609375 to 1
- capacity: int32 [128], replicated, may hold values from 128 to 383
- w_gate: bfloat16 [128, 4096, 768], P(('wide', 'narrow')), may hold values from -0.09375 to 0.09375
- w_up: bfloat16 [128, 4096, 768], P(('wide', 'narrow')), may hold values from -0.09375 to 0.09375
- w_down: bfloat16 [128, 768, 4096], P(('wide', 'narrow')), may hold values from -0.21875 to 0.21875
Outputs:
- mixed: bfloat16 [16384, 4096], P(('wide', 'narrow'))
The draws below stay inside these ranges and needn't reach their ends.
Inputs may be any that keep to these rules, and one draw needn't show every extreme that they name: `expert_ids`: the two experts of a token differ; among the tokens of one device no expert is named more than 3 times, and that many is reached.
All inputs are finite; a program needn't handle non-finite values.
Results may differ from the reference program's by a relative error of at most 0.0058.
Values may be sent and summed in bfloat16 or wider, within the bound.
No kernel may reach another device: no remote copies, remote signals or barrier semaphores. Data moves between devices by JAX's collectives and lax.ppermute only.
A program may use at most 128 MiB of HBM per device.

```python
import math
import jax
import jax.numpy as jnp
import numpy as np
from jax import lax

D = 4096
FF = 768
TOK_DEV = 128
TOKENS = 16384
EXPERTS = 128
MOST = 3


def with_ends(array, rng, least, largest):
    dims = array.shape
    place = [jax.random.randint(jax.random.fold_in(rng, axis), (), 0, dims[axis]) for axis in range(len(dims))]
    array = array.at[tuple(place)].set(least)
    longest = dims.index(max(dims))
    place[longest] = (place[longest] + 1) % dims[longest]
    return array.at[tuple(place)].set(largest)


def block_levels(stream_key, dims, pieces, low, high):
    factor_of = 1.0
    for dim, blocks in pieces:
        heights = jax.random.uniform(jax.random.fold_in(jax.random.fold_in(stream_key, 6), dim), (blocks,), jnp.float32, low / len(pieces), high / len(pieces))
        factor_of = factor_of * jnp.repeat(jnp.exp(heights), dims[dim] // blocks).reshape((-1,) + (1,) * (len(dims) - 1 - dim))
    return factor_of


def deal_out(own_key, own, number, rows, amount, top, bound, slope):
    order = jax.random.permutation(own_key, amount)
    packed, common = load_shares(amount, rows * top, bound, slope, True), load_shares(amount, rows * top, bound, slope, False)
    places = jnp.arange(amount)

    def named(tallies, turn):
        used = int((tallies > 0).sum())
        fixed = max(1, used // 4)
        passed = fixed + (places - fixed + turn * (used - fixed)) % max(1, amount - fixed)
        return jnp.zeros((amount,), jnp.int32).at[order[jnp.where(places < fixed, places, passed)]].set(jnp.asarray(tallies, jnp.int32))

    tallies = jnp.where(number % 4 == 0, named(packed, number // 4), named(common, number - number // 4 - 1))
    mixed = jax.random.permutation(jax.random.fold_in(own, 3), amount)
    donor, taker = mixed[0:amount // 2 * 2:2], mixed[1:amount // 2 * 2:2]
    slack = jnp.minimum(tallies[donor] - 1, bound - tallies[taker]) // 2
    slack = jnp.where((donor == order[0]) | (taker == order[0]) | (tallies[taker] == 0), 0, jnp.maximum(slack, 0))
    passed = jax.random.randint(jax.random.fold_in(own, 4), (amount // 2,), 0, 1 << 20) % (slack + 1)
    tallies = tallies.at[donor].add(-passed).at[taker].add(passed)
    labels = jnp.searchsorted(jnp.cumsum(tallies), jnp.arange(rows * top), side="right").astype(jnp.int32)
    listing = labels.reshape(top, rows).T
    listing = listing[jax.random.permutation(jax.random.fold_in(own, 1), rows)]
    turn = jax.random.randint(jax.random.fold_in(own, 2), (rows, 1), 0, top)
    return jnp.take_along_axis(listing, (jnp.arange(top)[None, :] + turn) % top, axis=1)


def load_shares(amount, total, reach, skew, full):
    loads = [(1 << 20) // math.isqrt(standing ** skew) + 1 for standing in range(1, amount + 1)]
    largest = reach if full else min(reach, max(-(-total // amount), total * loads[0] // sum(loads)))
    least = 1 if total - largest >= amount - 1 else 0
    counts, rest = [largest] + [least] * (amount - 1), total - largest - least * (amount - 1)
    while rest > 0:
        candidates = [i for i in range(1, amount) if counts[i] < largest] or [i for i in range(1, amount) if counts[i] < reach]
        whole, remaining = sum([loads[i] for i in candidates]), rest
        for i in candidates:
            addition = min(reach - counts[i], max(1, remaining * loads[i] // whole), rest)
            counts[i] = counts[i] + addition
            rest = rest - addition
    return np.array(counts)


def normal_values(key, extent, scale, limit, shards=(), kind=jnp.bfloat16):
    array = jax.random.normal(key, extent, jnp.float32) * scale
    if len(shards) > 0:
        array = block_levels(key, extent, shards, -0.22, 0.18) * array
    return jnp.clip(array, min=-limit, max=limit).astype(kind)


def setup_inputs(seed: int = 0) -> dict:
    splits = jax.random.split(jax.random.key(seed), 8)
    tokens = normal_values(splits[0], (TOKENS, D), 1.0, 6.0, ((0, 128),))
    expert_ids_keys = jax.random.split(jax.random.fold_in(splits[1], 1), TOKENS // TOK_DEV)
    expert_ids_turns = jax.random.permutation(jax.random.fold_in(splits[1], 3), TOKENS // TOK_DEV)
    expert_ids = jax.vmap(lambda own, number: deal_out(jax.random.fold_in(splits[1], 2), own, number, TOK_DEV, EXPERTS, 2, MOST, 2))(expert_ids_keys, expert_ids_turns).reshape((TOKENS, 2))
    gate_values = jnp.clip(0.099609375 + 0.9003906 * jax.random.uniform(splits[2], (TOKENS, 2), jnp.float32) ** block_levels(splits[2], (TOKENS, 2), ((0, 128),), -0.2, 0.2), 0.099609375, 1.0).astype(jnp.bfloat16)
    capacity = with_ends(jax.random.randint(splits[3], (EXPERTS,), TOK_DEV, 3 * TOK_DEV), jax.random.fold_in(splits[3], 1), TOK_DEV, (3 * TOK_DEV) - 1).astype(jnp.int32)
    w_gate = normal_values(splits[4], (EXPERTS, D, FF), D ** -0.5, 0.09375, ((0, 128),))
    w_up = normal_values(splits[5], (EXPERTS, D, FF), D ** -0.5, 0.09375, ((0, 128),))
    w_down = normal_values(splits[6], (EXPERTS, FF, D), FF ** -0.5, 0.21875, ((0, 128),))
    return {"tokens": tokens, "expert_ids": expert_ids, "gate_values": gate_values, "capacity": capacity, "w_gate": w_gate, "w_up": w_up, "w_down": w_down}


def expert_apply(token_rows, gate_matrix, up_matrix, down_matrix):
    gate_part = jnp.dot(token_rows, gate_matrix, preferred_element_type=jnp.float32)
    up_part = jnp.dot(token_rows, up_matrix, preferred_element_type=jnp.float32)
    hidden = (jax.nn.silu(gate_part) * up_part).astype(jnp.bfloat16)
    return jnp.dot(hidden, down_matrix, preferred_element_type=jnp.float32).astype(jnp.bfloat16)


def reference(tokens, expert_ids, gate_values, capacity, w_gate, w_up, w_down):
    assigns = 2 * TOKENS
    flat_ids = expert_ids.reshape(-1).astype(jnp.int32)
    onehot = (flat_ids[:, None] == jnp.arange(EXPERTS, dtype=jnp.int32)[None, :]).astype(jnp.int32)
    global_rank = jnp.sum((jnp.cumsum(onehot, axis=0) - onehot) * onehot, axis=1).astype(jnp.int32)
    kept_mask = global_rank < capacity[flat_ids]
    room_rows = 3 * TOK_DEV
    slot_index = jnp.where(kept_mask, global_rank, room_rows).astype(jnp.int32)
    table = jnp.full((EXPERTS, room_rows + 1), assigns, jnp.int32)
    table = table.at[flat_ids, slot_index].set(jnp.arange(assigns, dtype=jnp.int32))
    table = table[:, :room_rows]
    weights = gate_values.reshape(-1).astype(jnp.float32) * kept_mask.astype(jnp.float32)
    padded_weights = jnp.concatenate([weights, jnp.zeros((1,), jnp.float32)])
    padded_tokens = jnp.concatenate([tokens, jnp.zeros((1, D), jnp.bfloat16)], axis=0)

    def expert_step(summed, inputs):
        column, gate_matrix, up_matrix, down_matrix = inputs
        owners = (column // 2).astype(jnp.int32)
        token_rows = padded_tokens[owners]
        results = expert_apply(token_rows, gate_matrix, up_matrix, down_matrix)
        scaled = results.astype(jnp.float32) * padded_weights[column][:, None]
        return summed.at[owners].add(scaled), None

    start = jnp.zeros((TOKENS + 1, D), jnp.float32)
    summed, unused = lax.scan(expert_step, start, (table, w_gate, w_up, w_down))
    return summed[:TOKENS].astype(jnp.bfloat16)
```

```python
import functools

import jax
import jax.numpy as jnp
from jax import lax
from jax.experimental import pallas as pl
from jax.experimental.pallas import tpu as pltpu
from jax.sharding import PartitionSpec as P

AXES = ("wide", "narrow")
BF = jnp.bfloat16
F32 = jnp.float32
MIB = 2**20
LANES = 128
ANY = pl.BlockSpec(memory_space=pl.ANY)
VM = pl.BlockSpec(memory_space=pltpu.VMEM)
SM = pl.BlockSpec(memory_space=pltpu.SMEM)
CHUNKS = ((2, 1, 0),)


def named(ids_ref, experts):
    toks = ids_ref.shape[1]
    e = lax.broadcasted_iota(jnp.int32, (experts, toks), 0)
    first = ids_ref[0:1, :] == e
    second = ids_ref[1:2, :] == e
    both = jnp.where(first | second, 1.0, 0.0).astype(BF)
    earlier = lax.broadcasted_iota(jnp.int32, (toks, toks), 0) < lax.broadcasted_iota(
        jnp.int32, (toks, toks), 1
    )
    rank = jnp.dot(both, jnp.where(earlier, 1.0, 0.0).astype(BF), preferred_element_type=F32)
    return first, second, rank


def dispatch_kernel(slots, marked, ids_ref, tok_ref, out_ref):
    experts = out_ref.shape[0]
    first, second, rank = named(ids_ref, experts)
    mine = first | second
    width = tok_ref.shape[1]
    for i, slot in enumerate(slots):
        pick = jnp.where(mine & (rank == float(slot)), 1.0, 0.0).astype(BF)
        rows = jnp.dot(pick, tok_ref[...], preferred_element_type=F32)
        if marked == slot:
            count = jnp.sum(jnp.where(mine, 1.0, 0.0), axis=1, keepdims=True)
            mark = jnp.where(count == 0.0, 8.0, jnp.where(count == 1.0, 16.0, 32.0))
            rows = rows + jnp.where(count >= 3.0, 0.0, mark)
        per = width // LANES
        out_ref[:, i * per : (i + 1) * per, :] = rows.astype(BF).reshape(experts, per, LANES)


def ffn_kernel(slots, leads, nf, nd, look, *refs):
    cap_ref, ref = refs[0], list(refs[1:])
    counts_in = None if leads else ref.pop(0)
    x_hbm, wg_hbm, wu_hbm, wd_hbm = ref[:4]
    ref = ref[4:]
    out_ref = ref.pop(0)
    counts_out = ref.pop(0) if leads else None
    x3, xs, wg, wu, wd, hs, xsem, gsem, usem, dsem = ref
    n, per, ff = x_hbm.shape[0], xs.shape[1] // LANES, hs.shape[1]
    ft, dt = ff // nf, xs.shape[1] // nd
    loads = []
    for f in range(nf):
        cut = (slice(None), slice(f * ft, (f + 1) * ft))
        loads.append(pltpu.make_async_copy(wg_hbm.at[0, :, f * ft : (f + 1) * ft], wg.at[f], gsem.at[f]))
        loads.append(pltpu.make_async_copy(wu_hbm.at[0, :, f * ft : (f + 1) * ft], wu.at[f], usem.at[f]))
    for d in range(nd):
        loads.append(pltpu.make_async_copy(wd_hbm.at[0, :, d * dt : (d + 1) * dt], wd.at[d], dsem.at[d]))
    xload = pltpu.make_async_copy(x_hbm, x3, xsem.at[0])
    xload.start()
    for load in loads[:look]:
        load.start()
    xload.wait()

    def take(i):
        loads[i].wait()
        if i + look < len(loads):
            loads[i + look].start()

    for i in range(len(slots)):
        xs[i * n : (i + 1) * n, :] = x3[:, i * per : (i + 1) * per, :].reshape(n, per * LANES)
    if leads:
        at = slots.index(2)
        seen = xs[at * n : (at + 1) * n, 0:LANES].astype(F32)
        count = jnp.where(seen < 7.0, 3.0, jnp.where(seen < 12.0, 0.0, jnp.where(seen < 24.0, 1.0, 2.0)))
        counts_out[...] = count
    else:
        count = counts_in[...]
    below = lax.broadcasted_iota(jnp.int32, (n, n), 1) < lax.broadcasted_iota(jnp.int32, (n, n), 0)
    before = jnp.dot(
        jnp.where(below, 1.0, 0.0).astype(BF), count.astype(BF), preferred_element_type=F32
    )
    limit = cap_ref[lax.axis_index("wide") * lax.axis_size("narrow") + lax.axis_index("narrow")]
    limit = limit.astype(F32)
    for f in range(nf):
        take(2 * f)
        gate = jnp.dot(xs[...], wg[f], preferred_element_type=F32)
        take(2 * f + 1)
        up = jnp.dot(xs[...], wu[f], preferred_element_type=F32)
        hs[:, f * ft : (f + 1) * ft] = (gate / (1.0 + jnp.exp(-gate)) * up).astype(BF)
    for d in range(nd):
        take(2 * nf + d)
        y = jnp.dot(hs[...], wd[d], preferred_element_type=F32)
        for i, slot in enumerate(slots):
            kept = (count > float(slot)) & (before + float(slot) < limit)
            part = jnp.where(kept[:, 0:1], y[i * n : (i + 1) * n], 0.0).astype(BF)
            p0 = i * per + d * (dt // LANES)
            out_ref[:, p0 : p0 + dt // LANES, :] = part.reshape(n, dt // LANES, LANES)


def combine_kernel(chunks, ids_ref, gates_ref, *refs):
    answers, out_ref = refs[:-1], refs[-1]
    experts, _, lanes = answers[0].shape
    width = out_ref.shape[1]
    per = width // lanes
    first, second, rank = named(ids_ref, experts)
    gates = gates_ref[...].astype(F32)
    weight = jnp.where(first, gates[0:1, :], 0.0) + jnp.where(second, gates[1:2, :], 0.0)
    total = None
    for slots, answer in zip(chunks, answers):
        for i, slot in enumerate(slots):
            pick = jnp.where(rank == float(slot), weight, 0.0).astype(BF)
            rows = answer[:, i * per : (i + 1) * per, :].reshape(experts, width)
            term = lax.dot_general(
                pick, rows, (((0,), (0,)), ((), ())), preferred_element_type=F32
            )
            total = term if total is None else total + term
    out_ref[...] = total.astype(BF)


def exchange(value):
    return lax.all_to_all(value, AXES, split_axis=0, concat_axis=0, tiled=True)


def on_device(tokens, expert_ids, gate_values, capacity, w_gate, w_up, w_down):
    experts = capacity.shape[0]
    toks, width = tokens.shape
    ff = w_gate.shape[2]
    per = width // LANES
    ids = expert_ids.T
    gates = gate_values.T
    nf, nd, look = 3, 4, 4

    def dispatch(slots):
        return pl.pallas_call(
            functools.partial(dispatch_kernel, slots, 2),
            out_shape=jax.ShapeDtypeStruct((experts, len(slots) * per, LANES), BF),
            in_specs=[VM, VM],
            out_specs=VM,
            compiler_params=pltpu.CompilerParams(vmem_limit_bytes=24 * MIB),
            cost_estimate=pl.CostEstimate(
                flops=2 * len(slots) * experts * toks * width, bytes_accessed=3 * MIB, transcendentals=0
            ),
            name=f"dispatch_{slots[0]}",
        )(ids, tokens)

    def ffn(slots, arrived, counts):
        leads = counts is None
        rows = experts * len(slots)
        shape = jax.ShapeDtypeStruct(arrived.shape, BF)
        count_shape = jax.ShapeDtypeStruct((experts, LANES), F32)
        return pl.pallas_call(
            functools.partial(ffn_kernel, slots, leads, nf, nd, look),
            out_shape=(shape, count_shape) if leads else shape,
            in_specs=[SM] + ([] if leads else [VM]) + [ANY] * 4,
            out_specs=(VM, VM) if leads else VM,
            scratch_shapes=[
                pltpu.VMEM(arrived.shape, BF),
                pltpu.VMEM((rows, width), BF),
                pltpu.VMEM((nf, width, ff // nf), BF),
                pltpu.VMEM((nf, width, ff // nf), BF),
                pltpu.VMEM((nd, ff, width // nd), BF),
                pltpu.VMEM((rows, ff), BF),
                pltpu.SemaphoreType.DMA((1,)),
                pltpu.SemaphoreType.DMA((nf,)),
                pltpu.SemaphoreType.DMA((nf,)),
                pltpu.SemaphoreType.DMA((nd,)),
            ],
            compiler_params=pltpu.CompilerParams(vmem_limit_bytes=48 * MIB),
            cost_estimate=pl.CostEstimate(
                flops=6 * rows * width * ff, bytes_accessed=20 * MIB, transcendentals=rows * ff
            ),
            name=f"expert_{slots[0]}",
        )(*([capacity] + ([] if leads else [counts]) + [arrived, w_gate, w_up, w_down]))

    arrived = [exchange(dispatch(slots)) for slots in CHUNKS]
    answers, counts = [], None
    for slots, rows in zip(CHUNKS, arrived):
        if counts is None:
            rows, counts = ffn(slots, rows, None)
        else:
            rows = ffn(slots, rows, counts)
        answers.append(exchange(rows))
    return pl.pallas_call(
        functools.partial(combine_kernel, CHUNKS),
        out_shape=jax.ShapeDtypeStruct((toks, width), BF),
        in_specs=[VM] * (2 + len(answers)),
        out_specs=VM,
        compiler_params=pltpu.CompilerParams(vmem_limit_bytes=32 * MIB),
        cost_estimate=pl.CostEstimate(
            flops=6 * experts * toks * width, bytes_accessed=4 * MIB, transcendentals=0
        ),
        name="combine",
    )(ids, gates, *answers)


def solution(mesh):
    rows, whole = P(AXES, None), P(AXES, None, None)
    return jax.shard_map(
        on_device,
        mesh=mesh,
        in_specs=(rows, rows, rows, P(), whole, whole, whole),
        out_specs=rows,
        check_vma=False,
    )
```

```python
import functools

import jax
import jax.numpy as jnp
from jax import lax
from jax.experimental import pallas as pl
from jax.experimental.pallas import tpu as pltpu
from jax.sharding import PartitionSpec as P

AXES = ("wide", "narrow")
BF = jnp.bfloat16
F32 = jnp.float32
MIB = 2**20
LANES = 128
ANY = pl.BlockSpec(memory_space=pl.ANY)
VM = pl.BlockSpec(memory_space=pltpu.VMEM)
HB = pl.BlockSpec(memory_space=pltpu.HBM)
SM = pl.BlockSpec(memory_space=pltpu.SMEM)
SLOTS = 3
ND = 4
PARTS = 4
HINT0, HINT1 = 2 * 10**9, 2 * 10**9
DISPATCH_MIB, FFN_MIB, COMBINE_MIB = 12, 16, 12


def named(ids, experts):
    toks = ids.shape[1]
    e = lax.broadcasted_iota(jnp.int32, (experts, toks), 0)
    first = ids[0:1, :] == e
    second = ids[1:2, :] == e
    both = jnp.where(first | second, 1.0, 0.0).astype(BF)
    earlier = lax.broadcasted_iota(jnp.int32, (toks, toks), 0) < lax.broadcasted_iota(
        jnp.int32, (toks, toks), 1
    )
    rank = jnp.dot(both, jnp.where(earlier, 1.0, 0.0).astype(BF), preferred_element_type=F32)
    return first, second, rank


def route_kernel(ids_ref, picks_ref, mark_ref):
    experts = mark_ref.shape[0]
    first, second, rank = named(ids_ref[...], experts)
    mine = first | second
    for slot in range(SLOTS):
        pick = jnp.where(mine & (rank == float(slot)), 1.0, 0.0)
        picks_ref[slot * experts : (slot + 1) * experts, :] = pick.astype(BF)
    count = jnp.sum(jnp.where(mine, 1.0, 0.0), axis=1, keepdims=True)
    mark = jnp.where(count == 0.0, 8.0, jnp.where(count == 1.0, 16.0, 32.0))
    mark_ref[...] = jnp.broadcast_to(jnp.where(count >= 3.0, 0.0, mark), mark_ref.shape)


def dispatch_kernel(picks_ref, mark_ref, tok_ref, out_ref):
    experts, width = out_ref.shape[0], tok_ref.shape[1]
    wide = width // PARTS
    per, part = width // LANES, wide // LANES
    for c in range(PARTS):
        picked = jnp.dot(
            picks_ref[...], tok_ref[:, c * wide : (c + 1) * wide], preferred_element_type=F32
        )
        for slot in range(SLOTS):
            rows = picked[slot * experts : (slot + 1) * experts]
            if slot == SLOTS - 1:
                rows = rows + mark_ref[:, 0:1]
            p0 = slot * per + c * part
            out_ref[:, p0 : p0 + part, :] = rows.astype(BF).reshape(experts, part, LANES)


def ffn_kernel(nd, cap_ref, x_ref, wg_ref, wu_ref, wd_ref, out_ref, hs):
    n, width = x_ref.shape[0], wd_ref.shape[2]
    per, dt = width // LANES, width // nd
    x = jnp.concatenate(
        [x_ref[:, i * per : (i + 1) * per, :].reshape(n, width) for i in range(SLOTS)], axis=0
    )
    gate = jnp.dot(x, wg_ref[0], preferred_element_type=F32)
    up = jnp.dot(x, wu_ref[0], preferred_element_type=F32)
    hs[...] = (gate / (1.0 + jnp.exp(-gate)) * up).astype(BF)
    seen = x[(SLOTS - 1) * n :, 0:LANES].astype(F32)
    count = jnp.where(seen < 7.0, 3.0, jnp.where(seen < 12.0, 0.0, jnp.where(seen < 24.0, 1.0, 2.0)))
    below = lax.broadcasted_iota(jnp.int32, (n, n), 1) < lax.broadcasted_iota(jnp.int32, (n, n), 0)
    before = jnp.dot(
        jnp.where(below, 1.0, 0.0).astype(BF), count.astype(BF), preferred_element_type=F32
    )
    limit = cap_ref[lax.axis_index("wide") * lax.axis_size("narrow") + lax.axis_index("narrow")]
    limit = limit.astype(F32)
    for d in range(nd):
        y = jnp.dot(hs[...], wd_ref[0, :, d * dt : (d + 1) * dt], preferred_element_type=F32)
        for slot in range(SLOTS):
            kept = (count > float(slot)) & (before + float(slot) < limit)
            part = jnp.where(kept[:, 0:1], y[slot * n : (slot + 1) * n], 0.0).astype(BF)
            p0 = slot * per + d * (dt // LANES)
            out_ref[:, p0 : p0 + dt // LANES, :] = part.reshape(n, dt // LANES, LANES)


def combine_kernel(ids_ref, gates_ref, answer_ref, out_hbm, out_ref, sems):
    experts, parts = answer_ref.shape[0], out_ref.shape[0]
    wide = out_ref.shape[2]
    per, part = parts * wide // LANES, wide // LANES
    first, second, rank = named(ids_ref[...], experts)
    gates = gates_ref[...].astype(F32)
    weight = jnp.where(first, gates[0:1, :], 0.0) + jnp.where(second, gates[1:2, :], 0.0)
    picks = jnp.concatenate(
        [jnp.where(rank == float(slot), weight, 0.0).astype(BF) for slot in range(SLOTS)], axis=0
    )
    stores = []
    for c in range(parts):
        rows = jnp.concatenate(
            [
                answer_ref[:, p0 : p0 + part, :].reshape(experts, wide)
                for p0 in range(c * part, SLOTS * per, per)
            ],
            axis=0,
        )
        total = lax.dot_general(picks, rows, (((0,), (0,)), ((), ())), preferred_element_type=F32)
        out_ref[c] = total.astype(BF)
        store = pltpu.make_async_copy(out_ref.at[c], out_hbm.at[:, c * wide : (c + 1) * wide], sems.at[c])
        store.start()
        stores.append(store)
    for store in stores:
        store.wait()


def exchange(value):
    return lax.all_to_all(value, AXES, split_axis=0, concat_axis=0, tiled=True)


def on_device(tokens, expert_ids, gate_values, capacity, w_gate, w_up, w_down):
    experts = capacity.shape[0]
    toks, width = tokens.shape
    ff = w_gate.shape[2]
    rows = SLOTS * experts
    message = jax.ShapeDtypeStruct((experts, SLOTS * width // LANES, LANES), BF)
    ids = expert_ids.T
    gates = gate_values.T
    picks, mark = pl.pallas_call(
        route_kernel,
        out_shape=(
            jax.ShapeDtypeStruct((rows, toks), BF),
            jax.ShapeDtypeStruct((experts, LANES), F32),
        ),
        in_specs=[VM],
        out_specs=(VM, VM),
        compiler_params=pltpu.CompilerParams(vmem_limit_bytes=4 * MIB),
        cost_estimate=pl.CostEstimate(flops=HINT0, bytes_accessed=MIB, transcendentals=0),
        name="route",
    )(ids)
    outgoing = pl.pallas_call(
        dispatch_kernel,
        out_shape=message,
        in_specs=[VM, VM, VM],
        out_specs=VM,
        compiler_params=pltpu.CompilerParams(vmem_limit_bytes=DISPATCH_MIB * MIB),
        cost_estimate=pl.CostEstimate(flops=HINT1, bytes_accessed=4 * MIB, transcendentals=0),
        name="dispatch",
    )(picks, mark, tokens)
    arrived = exchange(outgoing)
    results = pl.pallas_call(
        functools.partial(ffn_kernel, ND),
        out_shape=message,
        in_specs=[SM] + [VM] * 4,
        out_specs=VM,
        scratch_shapes=[pltpu.VMEM((rows, ff), BF)],
        compiler_params=pltpu.CompilerParams(vmem_limit_bytes=FFN_MIB * MIB),
        cost_estimate=pl.CostEstimate(
            flops=6 * rows * width * ff, bytes_accessed=26 * MIB, transcendentals=rows * ff
        ),
        name="expert",
    )(capacity, arrived, w_gate, w_up, w_down)
    answers = exchange(results)
    return pl.pallas_call(
        combine_kernel,
        out_shape=jax.ShapeDtypeStruct((toks, width), BF),
        in_specs=[VM] * 3,
        out_specs=HB,
        scratch_shapes=[
            pltpu.VMEM((PARTS, toks, width // PARTS), BF),
            pltpu.SemaphoreType.DMA((PARTS,)),
        ],
        compiler_params=pltpu.CompilerParams(vmem_limit_bytes=COMBINE_MIB * MIB),
        cost_estimate=pl.CostEstimate(
            flops=2 * rows * toks * width, bytes_accessed=4 * MIB, transcendentals=0
        ),
        name="combine",
    )(ids, gates, answers)


def solution(mesh):
    rows, whole = P(AXES, None), P(AXES, None, None)
    return jax.shard_map(
        on_device,
        mesh=mesh,
        in_specs=(rows, rows, rows, P(), whole, whole, whole),
        out_specs=rows,
        check_vma=False,
    )
```

```python
import functools

import jax
import jax.numpy as jnp
from jax import lax
from jax.experimental import pallas as pl
from jax.experimental.pallas import tpu as pltpu
from jax.sharding import PartitionSpec as P

AXES = ("wide", "narrow")
BF = jnp.bfloat16
F32 = jnp.float32
MIB = 2**20
LANES = 128
ANY = pl.BlockSpec(memory_space=pl.ANY)
VM = pl.BlockSpec(memory_space=pltpu.VMEM)
HB = pl.BlockSpec(memory_space=pltpu.HBM)
SM = pl.BlockSpec(memory_space=pltpu.SMEM)
SLOTS = 3
ND = 4
PARTS = 4
HINT = 10**9
HINT0, HINT1 = 10**8, 6 * 10**9
DISPATCH_MIB, FFN_MIB, COMBINE_MIB = 12, 16, 12


def named(ids, experts):
    toks = ids.shape[1]
    e = lax.broadcasted_iota(jnp.int32, (experts, toks), 0)
    first = ids[0:1, :] == e
    second = ids[1:2, :] == e
    both = jnp.where(first | second, 1.0, 0.0).astype(BF)
    earlier = lax.broadcasted_iota(jnp.int32, (toks, toks), 0) < lax.broadcasted_iota(
        jnp.int32, (toks, toks), 1
    )
    rank = jnp.dot(both, jnp.where(earlier, 1.0, 0.0).astype(BF), preferred_element_type=F32)
    return first, second, rank


def first_kernel(out_ref):
    out_ref[...] = jnp.zeros(out_ref.shape, out_ref.dtype)


def route_kernel(ids_ref, first_ref, picks_ref, mark_ref):
    experts = mark_ref.shape[0]
    first, second, rank = named(ids_ref[...], experts)
    mine = first | second
    for slot in range(SLOTS):
        pick = jnp.where(mine & (rank == float(slot)), 1.0, 0.0)
        picks_ref[slot * experts : (slot + 1) * experts, :] = pick.astype(BF)
    count = jnp.sum(jnp.where(mine, 1.0, 0.0), axis=1, keepdims=True)
    mark = jnp.where(count == 0.0, 8.0, jnp.where(count == 1.0, 16.0, 32.0))
    mark_ref[...] = jnp.broadcast_to(jnp.where(count >= 3.0, 0.0, mark), mark_ref.shape)


def dispatch_kernel(picks_ref, mark_ref, tok_ref, out_ref):
    experts, width = out_ref.shape[0], tok_ref.shape[1]
    wide = width // PARTS
    per, part = width // LANES, wide // LANES
    for c in range(PARTS):
        picked = jnp.dot(
            picks_ref[...], tok_ref[:, c * wide : (c + 1) * wide], preferred_element_type=F32
        )
        for slot in range(SLOTS):
            rows = picked[slot * experts : (slot + 1) * experts]
            if slot == SLOTS - 1:
                rows = rows + mark_ref[:, 0:1]
            p0 = slot * per + c * part
            out_ref[:, p0 : p0 + part, :] = rows.astype(BF).reshape(experts, part, LANES)


def ffn_kernel(nd, cap_ref, x_ref, wg_ref, wu_ref, wd_ref, out_ref, hs):
    n, width = x_ref.shape[0], wd_ref.shape[2]
    per, dt = width // LANES, width // nd
    x = jnp.concatenate(
        [x_ref[:, i * per : (i + 1) * per, :].reshape(n, width) for i in range(SLOTS)], axis=0
    )
    gate = jnp.dot(x, wg_ref[0], preferred_element_type=F32)
    up = jnp.dot(x, wu_ref[0], preferred_element_type=F32)
    hs[...] = (gate / (1.0 + jnp.exp(-gate)) * up).astype(BF)
    seen = x[(SLOTS - 1) * n :, 0:LANES].astype(F32)
    count = jnp.where(seen < 7.0, 3.0, jnp.where(seen < 12.0, 0.0, jnp.where(seen < 24.0, 1.0, 2.0)))
    below = lax.broadcasted_iota(jnp.int32, (n, n), 1) < lax.broadcasted_iota(jnp.int32, (n, n), 0)
    before = jnp.dot(
        jnp.where(below, 1.0, 0.0).astype(BF), count.astype(BF), preferred_element_type=F32
    )
    limit = cap_ref[lax.axis_index("wide") * lax.axis_size("narrow") + lax.axis_index("narrow")]
    limit = limit.astype(F32)
    for d in range(nd):
        y = jnp.dot(hs[...], wd_ref[0, :, d * dt : (d + 1) * dt], preferred_element_type=F32)
        for slot in range(SLOTS):
            kept = (count > float(slot)) & (before + float(slot) < limit)
            part = jnp.where(kept[:, 0:1], y[slot * n : (slot + 1) * n], 0.0).astype(BF)
            p0 = slot * per + d * (dt // LANES)
            out_ref[:, p0 : p0 + dt // LANES, :] = part.reshape(n, dt // LANES, LANES)


def combine_kernel(ids_ref, gates_ref, answer_ref, out_hbm, out_ref, sems):
    experts, parts = answer_ref.shape[0], out_ref.shape[0]
    wide = out_ref.shape[2]
    per, part = parts * wide // LANES, wide // LANES
    first, second, rank = named(ids_ref[...], experts)
    gates = gates_ref[...].astype(F32)
    weight = jnp.where(first, gates[0:1, :], 0.0) + jnp.where(second, gates[1:2, :], 0.0)
    picks = jnp.concatenate(
        [jnp.where(rank == float(slot), weight, 0.0).astype(BF) for slot in range(SLOTS)], axis=0
    )
    stores = []
    for c in range(parts):
        rows = jnp.concatenate(
            [
                answer_ref[:, p0 : p0 + part, :].reshape(experts, wide)
                for p0 in range(c * part, SLOTS * per, per)
            ],
            axis=0,
        )
        total = lax.dot_general(picks, rows, (((0,), (0,)), ((), ())), preferred_element_type=F32)
        out_ref[c] = total.astype(BF)
        store = pltpu.make_async_copy(out_ref.at[c], out_hbm.at[:, c * wide : (c + 1) * wide], sems.at[c])
        store.start()
        stores.append(store)
    for store in stores:
        store.wait()


def exchange(value):
    return lax.all_to_all(value, AXES, split_axis=0, concat_axis=0, tiled=True)


def on_device(tokens, expert_ids, gate_values, capacity, w_gate, w_up, w_down):
    experts = capacity.shape[0]
    toks, width = tokens.shape
    ff = w_gate.shape[2]
    rows = SLOTS * experts
    message = jax.ShapeDtypeStruct((experts, SLOTS * width // LANES, LANES), BF)
    ids = expert_ids.T
    gates = gate_values.T
    first = pl.pallas_call(
        first_kernel,
        out_shape=jax.ShapeDtypeStruct((8, LANES), F32),
        out_specs=VM,
        compiler_params=pltpu.CompilerParams(vmem_limit_bytes=MIB),
        cost_estimate=pl.CostEstimate(flops=HINT, bytes_accessed=MIB, transcendentals=0),
        name="first",
    )()
    picks, mark = pl.pallas_call(
        route_kernel,
        out_shape=(
            jax.ShapeDtypeStruct((rows, toks), BF),
            jax.ShapeDtypeStruct((experts, LANES), F32),
        ),
        in_specs=[VM, VM],
        out_specs=(VM, VM),
        compiler_params=pltpu.CompilerParams(vmem_limit_bytes=4 * MIB),
        cost_estimate=pl.CostEstimate(flops=HINT0, bytes_accessed=MIB, transcendentals=0),
        name="route",
    )(ids, first)
    outgoing = pl.pallas_call(
        dispatch_kernel,
        out_shape=message,
        in_specs=[VM, VM, VM],
        out_specs=VM,
        compiler_params=pltpu.CompilerParams(vmem_limit_bytes=DISPATCH_MIB * MIB),
        cost_estimate=pl.CostEstimate(flops=HINT1, bytes_accessed=4 * MIB, transcendentals=0),
        name="dispatch",
    )(picks, mark, tokens)
    arrived = exchange(outgoing)
    results = pl.pallas_call(
        functools.partial(ffn_kernel, ND),
        out_shape=message,
        in_specs=[SM] + [VM] * 4,
        out_specs=VM,
        scratch_shapes=[pltpu.VMEM((rows, ff), BF)],
        compiler_params=pltpu.CompilerParams(vmem_limit_bytes=FFN_MIB * MIB),
        cost_estimate=pl.CostEstimate(
            flops=6 * rows * width * ff, bytes_accessed=26 * MIB, transcendentals=rows * ff
        ),
        name="expert",
    )(capacity, arrived, w_gate, w_up, w_down)
    answers = exchange(results)
    return pl.pallas_call(
        combine_kernel,
        out_shape=jax.ShapeDtypeStruct((toks, width), BF),
        in_specs=[VM] * 3,
        out_specs=HB,
        scratch_shapes=[
            pltpu.VMEM((PARTS, toks, width // PARTS), BF),
            pltpu.SemaphoreType.DMA((PARTS,)),
        ],
        compiler_params=pltpu.CompilerParams(vmem_limit_bytes=COMBINE_MIB * MIB),
        cost_estimate=pl.CostEstimate(
            flops=2 * rows * toks * width, bytes_accessed=4 * MIB, transcendentals=0
        ),
        name="combine",
    )(ids, gates, answers)


def solution(mesh):
    rows, whole = P(AXES, None), P(AXES, None, None)
    return jax.shard_map(
        on_device,
        mesh=mesh,
        in_specs=(rows, rows, rows, P(), whole, whole, whole),
        out_specs=rows,
        check_vma=False,
    )
```

```python
import functools

import jax
import jax.numpy as jnp
from jax import lax
from jax.experimental import pallas as pl
from jax.experimental.pallas import tpu as pltpu
from jax.sharding import PartitionSpec as P

AXES = ("wide", "narrow")
BF = jnp.bfloat16
F32 = jnp.float32
MIB = 2**20
LANES = 128
ANY = pl.BlockSpec(memory_space=pl.ANY)
VM = pl.BlockSpec(memory_space=pltpu.VMEM)
HB = pl.BlockSpec(memory_space=pltpu.HBM)
SM = pl.BlockSpec(memory_space=pltpu.SMEM)
SLOTS = 3
NF, ND = 3, 4
PARTS = 4
HINT = 10**9
HINT0, HINT1 = 10**8, 6 * 10**9
DISPATCH_MIB, FFN_MIB, COMBINE_MIB = 12, 16, 12


def named(ids, experts):
    toks = ids.shape[1]
    e = lax.broadcasted_iota(jnp.int32, (experts, toks), 0)
    first = ids[0:1, :] == e
    second = ids[1:2, :] == e
    both = jnp.where(first | second, 1.0, 0.0).astype(BF)
    earlier = lax.broadcasted_iota(jnp.int32, (toks, toks), 0) < lax.broadcasted_iota(
        jnp.int32, (toks, toks), 1
    )
    rank = jnp.dot(both, jnp.where(earlier, 1.0, 0.0).astype(BF), preferred_element_type=F32)
    return first, second, rank


def first_kernel(out_ref):
    out_ref[...] = jnp.zeros(out_ref.shape, out_ref.dtype)


def route_kernel(ids_ref, first_ref, picks_ref, mark_ref):
    experts = mark_ref.shape[0]
    first, second, rank = named(ids_ref[...], experts)
    mine = first | second
    for slot in range(SLOTS):
        pick = jnp.where(mine & (rank == float(slot)), 1.0, 0.0)
        picks_ref[slot * experts : (slot + 1) * experts, :] = pick.astype(BF)
    count = jnp.sum(jnp.where(mine, 1.0, 0.0), axis=1, keepdims=True)
    mark = jnp.where(count == 0.0, 8.0, jnp.where(count == 1.0, 16.0, 32.0))
    mark_ref[...] = jnp.broadcast_to(jnp.where(count >= 3.0, 0.0, mark), mark_ref.shape)


def dispatch_kernel(picks_ref, mark_ref, tok_ref, out_ref):
    experts, width = out_ref.shape[0], tok_ref.shape[1]
    wide = width // PARTS
    per, part = width // LANES, wide // LANES
    for c in range(PARTS):
        picked = jnp.dot(
            picks_ref[...], tok_ref[:, c * wide : (c + 1) * wide], preferred_element_type=F32
        )
        for slot in range(SLOTS):
            rows = picked[slot * experts : (slot + 1) * experts]
            if slot == SLOTS - 1:
                rows = rows + mark_ref[:, 0:1]
            p0 = slot * per + c * part
            out_ref[:, p0 : p0 + part, :] = rows.astype(BF).reshape(experts, part, LANES)


def ffn_kernel(nf, nd, cap_ref, x_ref, wg_ref, wu_ref, wd_ref, out_ref, xs, hs):
    n, width, ff = x_ref.shape[0], wd_ref.shape[2], hs.shape[1]
    per, ft, dt = width // LANES, ff // nf, width // nd
    for i in range(SLOTS):
        xs[i * n : (i + 1) * n, :] = x_ref[:, i * per : (i + 1) * per, :].reshape(n, width)
    seen = xs[(SLOTS - 1) * n : SLOTS * n, 0:LANES].astype(F32)
    count = jnp.where(seen < 7.0, 3.0, jnp.where(seen < 12.0, 0.0, jnp.where(seen < 24.0, 1.0, 2.0)))
    below = lax.broadcasted_iota(jnp.int32, (n, n), 1) < lax.broadcasted_iota(jnp.int32, (n, n), 0)
    before = jnp.dot(
        jnp.where(below, 1.0, 0.0).astype(BF), count.astype(BF), preferred_element_type=F32
    )
    limit = cap_ref[lax.axis_index("wide") * lax.axis_size("narrow") + lax.axis_index("narrow")]
    limit = limit.astype(F32)
    kept = jnp.concatenate(
        [
            jnp.where((count > float(slot)) & (before + float(slot) < limit), 1.0, 0.0)[:, 0:1]
            for slot in range(SLOTS)
        ],
        axis=0,
    )
    for f in range(nf):
        cut = slice(f * ft, (f + 1) * ft)
        gate = jnp.dot(xs[...], wg_ref[0, :, cut], preferred_element_type=F32)
        up = jnp.dot(xs[...], wu_ref[0, :, cut], preferred_element_type=F32)
        hidden = gate / (1.0 + jnp.exp(-gate)) * up
        hs[:, cut] = jnp.where(kept > 0.0, hidden, 0.0).astype(BF)
    for d in range(nd):
        y = jnp.dot(hs[...], wd_ref[0, :, d * dt : (d + 1) * dt], preferred_element_type=F32)
        for slot in range(SLOTS):
            part = y[slot * n : (slot + 1) * n].astype(BF)
            p0 = slot * per + d * (dt // LANES)
            out_ref[:, p0 : p0 + dt // LANES, :] = part.reshape(n, dt // LANES, LANES)


def combine_kernel(ids_ref, gates_ref, picks_ref, answer_ref, out_hbm, out_ref, sems):
    experts, parts = answer_ref.shape[0], out_ref.shape[0]
    wide = out_ref.shape[2]
    per, part = parts * wide // LANES, wide // LANES
    e = lax.broadcasted_iota(jnp.int32, (experts, ids_ref.shape[1]), 0)
    gates = gates_ref[...].astype(F32)
    weight = jnp.where(ids_ref[0:1, :] == e, gates[0:1, :], gates[1:2, :]).astype(BF)
    picks = jnp.concatenate(
        [picks_ref[i * experts : (i + 1) * experts, :] * weight for i in range(SLOTS)], axis=0
    )
    stores = []
    for c in range(parts):
        rows = jnp.concatenate(
            [
                answer_ref[:, p0 : p0 + part, :].reshape(experts, wide)
                for p0 in range(c * part, SLOTS * per, per)
            ],
            axis=0,
        )
        total = lax.dot_general(picks, rows, (((0,), (0,)), ((), ())), preferred_element_type=F32)
        out_ref[c] = total.astype(BF)
        store = pltpu.make_async_copy(out_ref.at[c], out_hbm.at[:, c * wide : (c + 1) * wide], sems.at[c])
        store.start()
        stores.append(store)
    for store in stores:
        store.wait()


def exchange(value):
    return lax.all_to_all(value, AXES, split_axis=0, concat_axis=0, tiled=True)


def on_device(tokens, expert_ids, gate_values, capacity, w_gate, w_up, w_down):
    experts = capacity.shape[0]
    toks, width = tokens.shape
    ff = w_gate.shape[2]
    rows = SLOTS * experts
    message = jax.ShapeDtypeStruct((experts, SLOTS * width // LANES, LANES), BF)
    ids = expert_ids.T
    gates = gate_values.T
    first = pl.pallas_call(
        first_kernel,
        out_shape=jax.ShapeDtypeStruct((8, LANES), F32),
        out_specs=VM,
        compiler_params=pltpu.CompilerParams(vmem_limit_bytes=MIB),
        cost_estimate=pl.CostEstimate(flops=HINT, bytes_accessed=MIB, transcendentals=0),
        name="first",
    )()
    picks, mark = pl.pallas_call(
        route_kernel,
        out_shape=(
            jax.ShapeDtypeStruct((rows, toks), BF),
            jax.ShapeDtypeStruct((experts, LANES), F32),
        ),
        in_specs=[VM, VM],
        out_specs=(VM, VM),
        compiler_params=pltpu.CompilerParams(vmem_limit_bytes=4 * MIB),
        cost_estimate=pl.CostEstimate(flops=HINT0, bytes_accessed=MIB, transcendentals=0),
        name="route",
    )(ids, first)
    outgoing = pl.pallas_call(
        dispatch_kernel,
        out_shape=message,
        in_specs=[VM, VM, VM],
        out_specs=VM,
        compiler_params=pltpu.CompilerParams(vmem_limit_bytes=DISPATCH_MIB * MIB),
        cost_estimate=pl.CostEstimate(flops=HINT1, bytes_accessed=4 * MIB, transcendentals=0),
        name="dispatch",
    )(picks, mark, tokens)
    arrived = exchange(outgoing)
    results = pl.pallas_call(
        functools.partial(ffn_kernel, NF, ND),
        out_shape=message,
        in_specs=[SM] + [VM] * 4,
        out_specs=VM,
        scratch_shapes=[pltpu.VMEM((rows, width), BF), pltpu.VMEM((rows, ff), BF)],
        compiler_params=pltpu.CompilerParams(vmem_limit_bytes=FFN_MIB * MIB),
        cost_estimate=pl.CostEstimate(
            flops=6 * rows * width * ff, bytes_accessed=26 * MIB, transcendentals=rows * ff
        ),
        name="expert",
    )(capacity, arrived, w_gate, w_up, w_down)
    answers = exchange(results)
    return pl.pallas_call(
        combine_kernel,
        out_shape=jax.ShapeDtypeStruct((toks, width), BF),
        in_specs=[VM] * 4,
        out_specs=HB,
        scratch_shapes=[
            pltpu.VMEM((PARTS, toks, width // PARTS), BF),
            pltpu.SemaphoreType.DMA((PARTS,)),
        ],
        compiler_params=pltpu.CompilerParams(vmem_limit_bytes=COMBINE_MIB * MIB),
        cost_estimate=pl.CostEstimate(
            flops=2 * rows * toks * width, bytes_accessed=4 * MIB, transcendentals=0
        ),
        name="combine",
    )(ids, gates, picks, answers)


def solution(mesh):
    rows, whole = P(AXES, None), P(AXES, None, None)
    return jax.shard_map(
        on_device,
        mesh=mesh,
        in_specs=(rows, rows, rows, P(), whole, whole, whole),
        out_specs=rows,
        check_vma=False,
    )
```
